128 devices in a mesh: lat: 4 (over y_hi, core), lon: 4 (over z_hi, y_lo), lev: 8 (over z_lo, x).
Axes of the slice: x: 4, y: 4 (y_hi: 2, y_lo: 2; y = y_hi * 2 + y_lo), z: 4 (z_hi: 2, z_lo: 2; z = z_hi * 2 + z_lo), core: 2. Of those that a mesh axis runs over, the one named last changes fastest.
Arguments:
- density: float32 [128, 16, 1024, 128], P('lat', 'lon', 'lev'), may hold values from 0.2 to 1.8
- crowding: float32 [128, 16, 1024, 128], P('lat', 'lon', 'lev'), may hold values from 0.5 to 2
Outputs:
- running_total: float32 [128, 16, 1024, 128], P('lat', 'lon', 'lev')
- density_end: float32 [128, 16, 1024, 128], P('lat', 'lon', 'lev')
The draws below stay inside these ranges and needn't reach their ends.
All inputs are finite; a program needn't handle non-finite values.
Results may differ from the reference program's by a relative error of at most 0.00002.
Values sent between devices are 32-bit elements; how exact they have to be, the bound alone decides.
A program may use at most 320 MiB of HBM per device.

```python
import jax
import jax.numpy as jnp
from jax import lax

GRID_J = 128
GRID_I = 16
GRID_K = 1024
LEVELS = 128
STEPS = 4


def level_of(stream_key, shape, split, smallest, largest):
    level, own = 1.0, jax.random.fold_in(stream_key, 6)
    for dim, shards_of in split:
        heights = jnp.exp(jax.random.uniform(jax.random.fold_in(own, dim), (shards_of,), jnp.float32, smallest / len(split), largest / len(split)))
        level = level * jnp.repeat(heights, shape[dim] // shards_of).reshape([-1 if axis == dim else 1 for axis in range(len(shape))])
    return level


def setup_inputs(seed: int = 0) -> dict:
    key_list = jax.random.split(jax.random.key(seed), 3)
    density = jnp.clip(0.2 + 1.5999999 * jax.random.uniform(key_list[0], (GRID_J, GRID_I, GRID_K, LEVELS), jnp.float32) ** level_of(key_list[0], (GRID_J, GRID_I, GRID_K, LEVELS), ((0, 4), (1, 4), (2, 8)), -0.2, 0.2), 0.2, 1.8)
    crowding = jnp.clip(0.5 + 1.5 * jax.random.uniform(key_list[1], (GRID_J, GRID_I, GRID_K, LEVELS), jnp.float32) ** level_of(key_list[1], (GRID_J, GRID_I, GRID_K, LEVELS), ((0, 4), (1, 4), (2, 8)), -0.2, 0.2), 0.5, 2.0)
    return dict(density=density, crowding=crowding)


def without_rim(values, dims):
    for dim in dims:
        values = lax.slice_in_dim(values, 1, values.shape[dim] - 1, axis=dim)
    return values


def shifted_cells(values, dim, start, dims):
    others = [other for other in dims if other != dim]
    values = without_rim(values, others)
    return lax.slice_in_dim(values, start, start + values.shape[dim] - 2, axis=dim)


def march_step(padded, crowding):
    middle = without_rim(padded, (0, 1, 2))
    lower = [shifted_cells(padded, dim, 0, (0, 1, 2)) for dim in (0, 1, 2)]
    upper = [shifted_cells(padded, dim, 2, (0, 1, 2)) for dim in (0, 1, 2)]
    spread = lower[0] + upper[0] + lower[1] + upper[1] + lower[2] + upper[2] - 6.0 * middle
    return middle + 0.1 * spread + 0.2 * middle * (1.0 - middle * crowding)


def reference(density, crowding):
    for step in range(STEPS):
        density = march_step(jnp.pad(density, ((1, 1), (1, 1), (1, 1), (0, 0)), mode="wrap"), crowding)
    running_total = jnp.cumsum(density, axis=1) / GRID_I
    return running_total, density
```

```python
import jax
import jax.numpy as jnp
from jax import lax
from jax.experimental import pallas as pl
from jax.experimental.pallas import tpu as pltpu
from jax.sharding import PartitionSpec as P

STEPS = 4
ROWS = 1
LAG = 2
AHEAD = 8
MESH = pl.DeviceIdType.MESH


def swap_kernel(
    sizes,
    d_hbm, c_hbm, run_hbm, end_hbm,
    even, odd, crowd, ghost, edge, there, below, totals, bases, run_own, run_there,
    z_send, z_recv, k_send, k_recv, p_send, p_recv, j_send, j_recv,
    in_send, in_recv, in_own, out_send, out_recv, base_send, base_recv,
    total_send, total_recv, write,
):
    n_lat, n_lon, n_lev, nj, ni, nk, cells = sizes
    half, blocks = nk // 2, nj // ROWS
    wide = 2 * ni
    a, b, m = lax.axis_index("lat"), lax.axis_index("lon"), lax.axis_index("lev")
    core, y_hi = lax.rem(a, 2), a // 2
    y_lo, z_hi = lax.rem(b, 2), b // 2
    h = lax.rem(y_lo + y_hi + m, 2)
    pair = b + 1 - 2 * y_lo
    peer_p = (a, pair, m)
    peer_z = (a, lax.rem(b + 2, n_lon), m)
    peer_k = (a, b, lax.rem(m + n_lev - 1 + 2 * h, n_lev))
    peer_c = (a + 1 - 2 * core, b, m)
    peer_j = (lax.rem(a + n_lat - 1 + 2 * core, n_lat), pair, m)
    states = (even, odd)

    barrier = pltpu.get_barrier_semaphore()
    peers = (peer_p, peer_z, peer_k, peer_c, peer_j)
    for peer in peers:
        pl.semaphore_signal(barrier, inc=1, device_id=peer, device_id_type=MESH)
    pl.semaphore_wait(barrier, len(peers))

    def first(block):
        return block * ROWS + (1 - core) * (nj - (2 * block + 1) * ROWS)

    def remote(src, dst, send, recv, peer):
        return pltpu.make_async_remote_copy(
            src_ref=src, dst_ref=dst, send_sem=send, recv_sem=recv,
            device_id=peer, device_id_type=MESH,
        )

    here = pl.ds(pl.multiple_of(half * h, 8), half)
    away = pl.ds(pl.multiple_of(half * (1 - h), 8), half)

    def bring_away(block):
        j = first(block)
        rows, padded = pl.ds(j, ROWS), pl.ds(j + 1, ROWS)
        mine, mine_in = pl.ds(1 + ni * y_lo, ni), pl.ds(ni * y_lo, ni)
        return (
            remote(d_hbm.at[rows, :, away], even.at[padded, mine], in_send.at[0, block], in_recv.at[0, block], peer_p),
            remote(c_hbm.at[rows, :, away], crowd.at[rows, mine_in], in_send.at[1, block], in_recv.at[1, block], peer_p),
        )

    def bring_own(block):
        j = first(block)
        rows, padded = pl.ds(j, ROWS), pl.ds(j + 1, ROWS)
        mine, mine_in = pl.ds(1 + ni * y_lo, ni), pl.ds(ni * y_lo, ni)
        return (
            pltpu.make_async_copy(d_hbm.at[rows, :, here], even.at[padded, mine], in_own.at[0, block]),
            pltpu.make_async_copy(c_hbm.at[rows, :, here], crowd.at[rows, mine_in], in_own.at[1, block]),
        )

    def start_bring(block):
        for copy in bring_away(block) + bring_own(block):
            copy.start()

    def wait_bring(block):
        for copy in bring_own(block):
            copy.wait()
        for copy in bring_away(block):
            copy.wait_recv()

    def face_copies(t, block):
        state, par, j = states[t % 2], t % 2, first(block)
        rows, padded = pl.ds(j, ROWS), pl.ds(j + 1, ROWS)
        return (
            remote(state.at[padded, 1], state.at[padded, wide + 1], z_send.at[par, 0, block], z_recv.at[par, 0, block], peer_z),
            remote(state.at[padded, wide], state.at[padded, 0], z_send.at[par, 1, block], z_recv.at[par, 1, block], peer_z),
            remote(edge.at[par, h, rows], ghost.at[par, 1 - h, rows], k_send.at[par, block], k_recv.at[par, block], peer_k),
            remote(edge.at[par, 1 - h, rows], ghost.at[par, h, rows], p_send.at[par, block], p_recv.at[par, block], peer_p),
        )

    def row_copy(t, side):
        state, par = states[t % 2], t % 2
        inner = pl.ds(1, wide)
        if side == 0:
            row, ring_row, peer = 1 + (1 - core) * (nj - 1), core * (nj + 1), peer_c
        else:
            row, ring_row, peer = 1 + core * (nj - 1), (1 - core) * (nj + 1), peer_j
        return remote(state.at[row, inner], state.at[ring_row, inner], j_send.at[par, side], j_recv.at[par, side], peer)

    def send_faces(t, block):
        for copy in face_copies(t, block):
            copy.start()

        @pl.when(block == 0)
        def _():
            row_copy(t, 0).start()

        @pl.when(block == blocks - 1)
        def _():
            row_copy(t, 1).start()

    def wait_faces(t, block):
        for copy in face_copies(t, block):
            copy.wait_recv()

        @pl.when(block == 0)
        def _():
            row_copy(t, 0).wait_recv()

        @pl.when(block == blocks - 1)
        def _():
            row_copy(t, 1).wait_recv()

    def sent_faces(t, block):
        for copy in face_copies(t, block):
            copy.wait_send()

        @pl.when(block == 0)
        def _():
            row_copy(t, 0).wait_send()

        @pl.when(block == blocks - 1)
        def _():
            row_copy(t, 1).wait_send()

    place = lax.broadcasted_iota(jnp.int32, (half, cells), 0)

    def arrive(block):
        wait_bring(block)
        for row in range(ROWS):
            j = first(block) + row
            for i in range(wide):
                edge[0, 0, j, i : i + 1, :] = even[j + 1, i + 1, 0:1, :]
                edge[0, 1, j, i : i + 1, :] = even[j + 1, i + 1, half - 1 : half, :]
        send_faces(0, block)

    def step(t, block):
        old, new, par = states[(t - 1) % 2], states[t % 2], (t - 1) % 2
        wait_faces(t - 1, block)
        if t >= 2:
            sent_faces(t - 2, block)
        for row in range(ROWS):
            j = first(block) + row
            r = j + 1
            lower, middle = old[r, 0], old[r, 1]
            for i in range(wide):
                upper = old[r, i + 2]
                low = jnp.where(place == 0, ghost[par, 0, j, i : i + 1, :], pltpu.roll(middle, 1, 0))
                high = jnp.where(place == half - 1, ghost[par, 1, j, i : i + 1, :], pltpu.roll(middle, half - 1, 0))
                around = (lower + upper) + (old[r - 1, i + 1] + old[r + 1, i + 1]) + (low + high)
                value = 0.1 * around + middle * (0.6 - 0.2 * (crowd[j, i] * middle))
                new[r, i + 1] = value
                if t < STEPS:
                    edge[t % 2, 0, j, i : i + 1, :] = value[0:1]
                    edge[t % 2, 1, j, i : i + 1, :] = value[half - 1 : half]
                lower, middle = middle, upper
        if t < STEPS:
            send_faces(t, block)

    final = states[STEPS % 2]

    def out_copy(block):
        j = first(block)
        theirs = pl.ds(1 + ni * (1 - y_lo), ni)
        return remote(final.at[pl.ds(j + 1, ROWS), theirs], there.at[pl.ds(j, ROWS)], out_send.at[block], out_recv.at[block], peer_p)

    def own_copy(block):
        j = first(block)
        mine = pl.ds(1 + ni * y_lo, ni)
        return pltpu.make_async_copy(final.at[pl.ds(j + 1, ROWS), mine], end_hbm.at[pl.ds(j, ROWS), :, here], write.at[0, block])

    def total_copy(block):
        rows = pl.ds(first(block), ROWS)
        return remote(totals.at[rows], below.at[rows], total_send.at[block], total_recv.at[block], peer_z)

    def base_copy(block):
        rows = pl.ds(first(block), ROWS)
        return remote(bases.at[0, rows], bases.at[1, rows], base_send.at[block], base_recv.at[block], peer_p)

    def run_own_copy(block):
        rows = pl.ds(first(block), ROWS)
        return pltpu.make_async_copy(run_own.at[rows], run_hbm.at[rows, :, here], write.at[1, block])

    def there_copies(block):
        rows = pl.ds(first(block), ROWS)
        return (
            pltpu.make_async_copy(there.at[rows], end_hbm.at[rows, :, away], write.at[2, block]),
            pltpu.make_async_copy(run_there.at[rows], run_hbm.at[rows, :, away], write.at[3, block]),
        )

    def finish(block):
        out_copy(block).start()
        own_copy(block).start()

        @pl.when(z_hi == 0)
        def _():
            for row in range(ROWS):
                j = first(block) + row
                total = final[j + 1, 1]
                for i in range(1, wide):
                    total = total + final[j + 1, i + 1]
                totals[j] = total
                below[j] = jnp.zeros_like(total)
            total_copy(block).start()

    def sums(block):
        @pl.when(z_hi == 1)
        def _():
            total_copy(block).wait_recv()

        sent_faces(STEPS - 1, block)
        for row in range(ROWS):
            j = first(block) + row
            base = below[j]
            lowest = final[j + 1, 1]
            for i in range(1, ni):
                lowest = lowest + final[j + 1, i + 1]
            bases[0, j] = base + jnp.where(y_lo == 0, lowest, 0.0)
            run = base + jnp.where(y_lo == 1, lowest, 0.0)
            for i in range(ni):
                run = run + final[j + 1, 1 + ni * y_lo + i]
                run_own[j, i] = run * (1.0 / (ni * n_lon))
        base_copy(block).start()
        run_own_copy(block).start()

    def returned(block):
        out_copy(block).wait_recv()
        base_copy(block).wait_recv()
        for row in range(ROWS):
            j = first(block) + row
            run = bases[1, j]
            for i in range(ni):
                run = run + there[j, i]
                run_there[j, i] = run * (1.0 / (ni * n_lon))
        for copy in there_copies(block):
            copy.start()

    def guarded(stage, block):
        @pl.when((block >= 0) & (block < blocks))
        def _():
            stage(block)

    def close(block):
        for copy in bring_away(block):
            copy.wait_send()
        out_copy(block).wait_send()
        base_copy(block).wait_send()

        @pl.when(z_hi == 0)
        def _():
            total_copy(block).wait_send()

        own_copy(block).wait()
        run_own_copy(block).wait()
        for copy in there_copies(block):
            copy.wait()

    lax.fori_loop(0, min(AHEAD, blocks), lambda n, _: (start_bring(n), 0)[1], 0)

    def tick(n, carry):
        @pl.when(n + AHEAD < blocks)
        def _():
            start_bring(n + AHEAD)

        guarded(returned, n - LAG * (STEPS + 2))
        guarded(sums, n - LAG * (STEPS + 1))

        def last(block):
            step(STEPS, block)
            finish(block)

        guarded(last, n - LAG * STEPS)
        for t in range(STEPS - 1, 0, -1):
            guarded(lambda block, t=t: step(t, block), n - LAG * t)
        guarded(arrive, n)
        return carry

    lax.fori_loop(0, blocks + LAG * (STEPS + 2), tick, 0)
    lax.fori_loop(0, blocks, lambda n, _: (close(n), 0)[1], 0)


def solution(mesh):
    n_lat, n_lon, n_lev = (mesh.shape[axis] for axis in ("lat", "lon", "lev"))

    def body(density, crowding):
        nj, ni, nk, cells = density.shape
        half, blocks, wide = nk // 2, nj // ROWS, 2 * ni
        f32, dma = jnp.float32, pltpu.SemaphoreType.DMA
        out = jax.ShapeDtypeStruct(density.shape, f32)
        vmem = [
            (nj + 2, wide + 2, half, cells),
            (nj + 2, wide + 2, half, cells),
            (nj, wide, half, cells),
            (2, 2, nj, wide, cells),
            (2, 2, nj, wide, cells),
            (nj, ni, half, cells),
            (nj, half, cells),
            (nj, half, cells),
            (2, nj, half, cells),
            (nj, ni, half, cells),
            (nj, ni, half, cells),
        ]
        sems = [
            (2, 2, blocks), (2, 2, blocks), (2, blocks), (2, blocks), (2, blocks), (2, blocks), (2, 2), (2, 2),
            (2, blocks), (2, blocks), (2, blocks), (blocks,), (blocks,), (blocks,), (blocks,),
            (blocks,), (blocks,), (4, blocks),
        ]
        sizes = (n_lat, n_lon, n_lev, nj, ni, nk, cells)
        anywhere = pl.BlockSpec(memory_space=pl.ANY)

        def kernel(*refs):
            swap_kernel(sizes, *refs)

        return pl.pallas_call(
            kernel,
            out_shape=(out, out),
            in_specs=[anywhere, anywhere],
            out_specs=(anywhere, anywhere),
            scratch_shapes=[pltpu.VMEM(shape, f32) for shape in vmem] + [dma(shape) for shape in sems],
            compiler_params=pltpu.CompilerParams(
                collective_id=0, has_side_effects=True, vmem_limit_bytes=67043328
            ),
            cost_estimate=pl.CostEstimate(flops=14 * STEPS * density.size, bytes_accessed=16 * density.size, transcendentals=0),
            name="swap_sweep",
        )(density, crowding)

    spec = P("lat", "lon", "lev", None)
    return jax.shard_map(body, mesh=mesh, in_specs=(spec, spec), out_specs=(spec, spec), check_vma=False)
```

```python
import jax
import jax.numpy as jnp
from jax import lax
from jax.experimental import pallas as pl
from jax.experimental.pallas import tpu as pltpu
from jax.sharding import PartitionSpec as P

STEPS = 4
ROWS = 1
LAG = 3
AHEAD = 2
PIECES = 4
MESH = pl.DeviceIdType.MESH


def swap_kernel(
    sizes,
    d_hbm, c_hbm, run_out, end_out,
    even, odd, crowd, ghost, edge, below, totals, bases,
    z_send, z_recv, k_send, k_recv, p_send, p_recv, j_send, j_recv,
    in_send, in_recv, in_own, out_send, out_recv, base_send, base_recv,
    total_send, total_recv,
):
    n_lat, n_lon, n_lev, nj, ni, nk, cells = sizes
    half, blocks = nk // 2, nj // ROWS
    wide = 2 * ni
    a, b, m = lax.axis_index("lat"), lax.axis_index("lon"), lax.axis_index("lev")
    core, y_hi = lax.rem(a, 2), a // 2
    y_lo, z_hi = lax.rem(b, 2), b // 2
    h = lax.rem(y_lo + y_hi + m, 2)
    pair = b + 1 - 2 * y_lo
    peer_p = (a, pair, m)
    peer_z = (a, lax.rem(b + 2, n_lon), m)
    peer_k = (a, b, lax.rem(m + n_lev - 1 + 2 * h, n_lev))
    peer_c = (a + 1 - 2 * core, b, m)
    peer_j = (lax.rem(a + n_lat - 1 + 2 * core, n_lat), pair, m)
    states = (even, odd)

    barrier = pltpu.get_barrier_semaphore()
    peers = (peer_p, peer_z, peer_k, peer_c, peer_j)
    for peer in peers:
        pl.semaphore_signal(barrier, inc=1, device_id=peer, device_id_type=MESH)
    pl.semaphore_wait(barrier, len(peers))

    def first(block):
        return block * ROWS + (1 - core) * (nj - (2 * block + 1) * ROWS)

    def remote(src, dst, send, recv, peer):
        return pltpu.make_async_remote_copy(
            src_ref=src, dst_ref=dst, send_sem=send, recv_sem=recv,
            device_id=peer, device_id_type=MESH,
        )

    here = pl.ds(pl.multiple_of(half * h, 8), half)
    away = pl.ds(pl.multiple_of(half * (1 - h), 8), half)

    def bring_away(block):
        j = first(block)
        rows, padded = pl.ds(j, ROWS), pl.ds(j + 1, ROWS)
        mine, mine_in = pl.ds(1 + ni * y_lo, ni), pl.ds(ni * y_lo, ni)
        return (
            remote(d_hbm.at[rows, :, away], even.at[padded, mine], in_send.at[0, block], in_recv.at[0, block], peer_p),
            remote(c_hbm.at[rows, :, away], crowd.at[rows, mine_in], in_send.at[1, block], in_recv.at[1, block], peer_p),
        )

    def bring_own(block):
        j = first(block)
        rows, padded = pl.ds(j, ROWS), pl.ds(j + 1, ROWS)
        mine, mine_in = pl.ds(1 + ni * y_lo, ni), pl.ds(ni * y_lo, ni)
        return (
            pltpu.make_async_copy(d_hbm.at[rows, :, here], even.at[padded, mine], in_own.at[0, block]),
            pltpu.make_async_copy(c_hbm.at[rows, :, here], crowd.at[rows, mine_in], in_own.at[1, block]),
        )

    def start_bring(block):
        for copy in bring_away(block) + bring_own(block):
            copy.start()

    def wait_bring(block):
        for copy in bring_own(block):
            copy.wait()
        for copy in bring_away(block):
            copy.wait_recv()

    def face_copies(t, block):
        state, par, j = states[t % 2], t % 2, first(block)
        rows, padded = pl.ds(j, ROWS), pl.ds(j + 1, ROWS)
        return (
            remote(state.at[padded, 1], state.at[padded, wide + 1], z_send.at[par, 0, block], z_recv.at[par, 0, block], peer_z),
            remote(state.at[padded, wide], state.at[padded, 0], z_send.at[par, 1, block], z_recv.at[par, 1, block], peer_z),
            remote(edge.at[par, h, rows], ghost.at[par, 1 - h, rows], k_send.at[par, block], k_recv.at[par, block], peer_k),
            remote(edge.at[par, 1 - h, rows], ghost.at[par, h, rows], p_send.at[par, block], p_recv.at[par, block], peer_p),
        )

    def row_copy(t, side):
        state, par = states[t % 2], t % 2
        inner = pl.ds(1, wide)
        if side == 0:
            row, ring_row, peer = 1 + (1 - core) * (nj - 1), core * (nj + 1), peer_c
        else:
            row, ring_row, peer = 1 + core * (nj - 1), (1 - core) * (nj + 1), peer_j
        return remote(state.at[row, inner], state.at[ring_row, inner], j_send.at[par, side], j_recv.at[par, side], peer)

    def send_faces(t, block):
        for copy in face_copies(t, block):
            copy.start()

        @pl.when(block == 0)
        def _():
            row_copy(t, 0).start()

        @pl.when(block == blocks - 1)
        def _():
            row_copy(t, 1).start()

    def wait_faces(t, block):
        for copy in face_copies(t, block):
            copy.wait_recv()

        @pl.when(block == 0)
        def _():
            row_copy(t, 0).wait_recv()

        @pl.when(block == blocks - 1)
        def _():
            row_copy(t, 1).wait_recv()

    def sent_faces(t, block):
        for copy in face_copies(t, block):
            copy.wait_send()

        @pl.when(block == 0)
        def _():
            row_copy(t, 0).wait_send()

        @pl.when(block == blocks - 1)
        def _():
            row_copy(t, 1).wait_send()

    place = lax.broadcasted_iota(jnp.int32, (half, cells), 0)

    def arrive(block):
        wait_bring(block)
        for row in range(ROWS):
            j = first(block) + row
            for i in range(wide):
                edge[0, 0, j, i : i + 1, :] = even[j + 1, i + 1, 0:1, :]
                edge[0, 1, j, i : i + 1, :] = even[j + 1, i + 1, half - 1 : half, :]
        send_faces(0, block)

    def step(t, block):
        old, new, par = states[(t - 1) % 2], states[t % 2], (t - 1) % 2
        wait_faces(t - 1, block)
        if t >= 2:
            sent_faces(t - 2, block)
        for row in range(ROWS):
            j = first(block) + row
            r = j + 1
            lower, middle = old[r, 0], old[r, 1]
            for i in range(wide):
                upper = old[r, i + 2]
                low = jnp.where(place == 0, ghost[par, 0, j, i : i + 1, :], pltpu.roll(middle, 1, 0))
                high = jnp.where(place == half - 1, ghost[par, 1, j, i : i + 1, :], pltpu.roll(middle, half - 1, 0))
                around = (lower + upper) + (old[r - 1, i + 1] + old[r + 1, i + 1]) + (low + high)
                value = 0.1 * around + middle * (0.6 - 0.2 * (crowd[j, i] * middle))
                new[r, i + 1] = value
                if t < STEPS:
                    edge[t % 2, 0, j, i : i + 1, :] = value[0:1]
                    edge[t % 2, 1, j, i : i + 1, :] = value[half - 1 : half]
                lower, middle = middle, upper
        if t < STEPS:
            send_faces(t, block)

    final = states[STEPS % 2]

    def out_copy(block):
        j = first(block)
        theirs = pl.ds(1 + ni * (1 - y_lo), ni)
        return remote(final.at[pl.ds(j + 1, ROWS), theirs], end_out.at[pl.ds(j, ROWS), :, here], out_send.at[block], out_recv.at[block], peer_p)

    def total_copy(block):
        rows = pl.ds(first(block), ROWS)
        return remote(totals.at[rows], below.at[rows], total_send.at[block], total_recv.at[block], peer_z)

    def base_copy(block):
        rows = pl.ds(first(block), ROWS)
        return remote(bases.at[0, rows], bases.at[1, rows], base_send.at[block], base_recv.at[block], peer_p)

    def finish(block):
        out_copy(block).start()

        @pl.when(z_hi == 0)
        def _():
            for row in range(ROWS):
                j = first(block) + row
                total = final[j + 1, 1]
                for i in range(1, wide):
                    total = total + final[j + 1, i + 1]
                totals[j] = total
                below[j] = jnp.zeros_like(total)
            total_copy(block).start()

    def sums(block):
        @pl.when(z_hi == 1)
        def _():
            total_copy(block).wait_recv()

        sent_faces(STEPS - 1, block)
        for row in range(ROWS):
            j = first(block) + row
            base = below[j]
            lowest = final[j + 1, 1]
            for i in range(1, ni):
                lowest = lowest + final[j + 1, i + 1]
            bases[0, j] = base + jnp.where(y_lo == 0, lowest, 0.0)
            run = base + jnp.where(y_lo == 1, lowest, 0.0)
            for i in range(ni):
                value = final[j + 1, 1 + ni * y_lo + i]
                end_out[j, i, here] = value
                run = run + value
                run_out[j, i, here] = run * (1.0 / (ni * n_lon))
        base_copy(block).start()

    def returned(block):
        out_copy(block).wait_recv()
        base_copy(block).wait_recv()
        for row in range(ROWS):
            j = first(block) + row
            run = bases[1, j]
            for i in range(ni):
                run = run + end_out[j, i, away]
                run_out[j, i, away] = run * (1.0 / (ni * n_lon))

    def guarded(stage, block):
        @pl.when((block >= 0) & (block < blocks))
        def _():
            stage(block)

    def close(block):
        for copy in bring_away(block):
            copy.wait_send()
        out_copy(block).wait_send()
        base_copy(block).wait_send()

        @pl.when(z_hi == 0)
        def _():
            total_copy(block).wait_send()

    lax.fori_loop(0, min(AHEAD, blocks), lambda n, _: (start_bring(n), 0)[1], 0)

    def tick(n, carry):
        @pl.when(n + AHEAD < blocks)
        def _():
            start_bring(n + AHEAD)

        guarded(returned, n - LAG * (STEPS + 2))
        guarded(sums, n - LAG * (STEPS + 1))

        def last(block):
            step(STEPS, block)
            finish(block)

        guarded(last, n - LAG * STEPS)
        for t in range(STEPS - 1, 0, -1):
            guarded(lambda block, t=t: step(t, block), n - LAG * t)
        guarded(arrive, n)
        return carry

    lax.fori_loop(0, blocks + LAG * (STEPS + 2), tick, 0)
    lax.fori_loop(0, blocks, lambda n, _: (close(n), 0)[1], 0)


def flush_kernel(run_in, end_in, run_out, end_out, sems):
    copies = []
    for k in range(PIECES):
        size = run_in.shape[0] // PIECES
        rows = pl.ds(k * size, size)
        copies.append(pltpu.make_async_copy(run_in.at[rows], run_out.at[rows], sems.at[0, k]))
        copies.append(pltpu.make_async_copy(end_in.at[rows], end_out.at[rows], sems.at[1, k]))
    for copy in copies:
        copy.start()
    for copy in copies:
        copy.wait()


def solution(mesh):
    n_lat, n_lon, n_lev = (mesh.shape[axis] for axis in ("lat", "lon", "lev"))

    def body(density, crowding):
        nj, ni, nk, cells = density.shape
        half, blocks, wide = nk // 2, nj // ROWS, 2 * ni
        f32, dma = jnp.float32, pltpu.SemaphoreType.DMA
        out = pltpu.VMEM(density.shape, f32)
        vmem = [
            (nj + 2, wide + 2, half, cells),
            (nj + 2, wide + 2, half, cells),
            (nj, wide, half, cells),
            (2, 2, nj, wide, cells),
            (2, 2, nj, wide, cells),
            (nj, half, cells),
            (nj, half, cells),
            (2, nj, half, cells),
        ]
        sems = [
            (2, 2, blocks), (2, 2, blocks), (2, blocks), (2, blocks), (2, blocks), (2, blocks), (2, 2), (2, 2),
            (2, blocks), (2, blocks), (2, blocks), (blocks,), (blocks,), (blocks,), (blocks,),
            (blocks,), (blocks,),
        ]
        sizes = (n_lat, n_lon, n_lev, nj, ni, nk, cells)
        anywhere = pl.BlockSpec(memory_space=pl.ANY)
        inside = pl.BlockSpec(memory_space=pltpu.VMEM)

        def kernel(*refs):
            swap_kernel(sizes, *refs)

        results = pl.pallas_call(
            kernel,
            out_shape=(out, out),
            in_specs=[anywhere, anywhere],
            out_specs=(inside, inside),
            scratch_shapes=[pltpu.VMEM(shape, f32) for shape in vmem] + [dma(shape) for shape in sems],
            compiler_params=pltpu.CompilerParams(
                collective_id=0, has_side_effects=True, vmem_limit_bytes=48 * 1024 * 1024 - 8 * 1024 * 128
            ),
            cost_estimate=pl.CostEstimate(flops=14 * STEPS * density.size, bytes_accessed=16 * density.size, transcendentals=0),
            name="swap_sweep",
        )(density, crowding)
        whole = jax.ShapeDtypeStruct(density.shape, f32)
        return pl.pallas_call(
            flush_kernel,
            out_shape=(whole, whole),
            in_specs=[inside, inside],
            out_specs=(anywhere, anywhere),
            scratch_shapes=[dma((2, PIECES))],
            compiler_params=pltpu.CompilerParams(vmem_limit_bytes=1024 * 1024),
            cost_estimate=pl.CostEstimate(flops=density.size, bytes_accessed=16 * density.size, transcendentals=0),
            name="flush",
        )(*results)

    spec = P("lat", "lon", "lev", None)
    return jax.shard_map(body, mesh=mesh, in_specs=(spec, spec), out_specs=(spec, spec), check_vma=False)
```

```python
import jax
import jax.numpy as jnp
from jax import lax
from jax.experimental import pallas as pl
from jax.experimental.pallas import tpu as pltpu
from jax.sharding import PartitionSpec as P

STEPS = 4
ROWS = 1
LAG = 3
LAST = 2
AHEAD = 1
PIECES = 4
LOADS = 4
MESH = pl.DeviceIdType.MESH


def swap_kernel(
    sizes,
    d_hbm, c_hbm, run_out, end_out,
    even, odd, crowd, ghost, edge, below, totals, bases,
    z_send, z_recv, k_send, k_recv, j_send, j_recv,
    in_send, in_recv, in_own, out_send, out_recv, base_send, base_recv,
    total_send, total_recv,
):
    n_lat, n_lon, n_lev, nj, ni, nk, cells = sizes
    half, blocks = nk // 2, nj // ROWS
    wide = 2 * ni
    a, b, m = lax.axis_index("lat"), lax.axis_index("lon"), lax.axis_index("lev")
    core, y_hi = lax.rem(a, 2), a // 2
    y_lo, z_hi = lax.rem(b, 2), b // 2
    h = lax.rem(y_lo + y_hi, 2)
    pair = b + 1 - 2 * y_lo
    peer_p = (a, pair, m)
    peer_z = (a, lax.rem(b + 2, n_lon), m)
    peer_k = ((a, b, lax.rem(m + n_lev - 1, n_lev)), (a, b, lax.rem(m + 1, n_lev)))
    peer_c = (a + 1 - 2 * core, b, m)
    peer_j = (lax.rem(a + n_lat - 1 + 2 * core, n_lat), pair, m)
    states = (even, odd)

    barrier = pltpu.get_barrier_semaphore()
    peers = (peer_p, peer_z, *peer_k, peer_c, peer_j)
    for peer in peers:
        pl.semaphore_signal(barrier, inc=1, device_id=peer, device_id_type=MESH)

    def first(block):
        return block * ROWS + (1 - core) * (nj - (2 * block + 1) * ROWS)

    def remote(src, dst, send, recv, peer):
        return pltpu.make_async_remote_copy(
            src_ref=src, dst_ref=dst, send_sem=send, recv_sem=recv,
            device_id=peer, device_id_type=MESH,
        )

    here = pl.ds(pl.multiple_of(half * h, 8), half)
    away = pl.ds(pl.multiple_of(half * (1 - h), 8), half)
    lane = lax.broadcasted_iota(jnp.int32, (half, cells), 1)
    mine = jnp.where(lane >= cells // 2, 1, 0) == h
    place = lax.broadcasted_iota(jnp.int32, (half, cells), 0)
    left = lax.broadcasted_iota(jnp.int32, (wide, cells), 1) < cells // 2

    def swing(value):
        return pltpu.roll(value, cells // 2, 1)

    def load(block):
        rows = pl.ds(first(block), ROWS)
        return (
            pltpu.make_async_copy(d_hbm.at[rows], end_out.at[rows], in_own.at[0, block]),
            pltpu.make_async_copy(c_hbm.at[rows], run_out.at[rows], in_own.at[1, block]),
        )

    def start_load(block):
        for copy in load(block):
            copy.start()

    def pack(block):
        for copy in load(block):
            copy.wait()
        for row in range(ROWS):
            j = first(block) + row
            for q in range(ni):
                for source, kept in (
                    (end_out, even.at[j + 1, 1 + ni * y_lo + q]),
                    (run_out, crowd.at[j, ni * y_lo + q]),
                ):
                    near, far = source[j, q, here], source[j, q, away]
                    kept[...] = jnp.where(mine, near, swing(far))
                    source[j, q, 0:half] = jnp.where(mine, swing(near), far)

    def give(block):
        j = first(block)
        rows, padded = pl.ds(j, ROWS), pl.ds(j + 1, ROWS)
        packed = pl.ds(0, half)
        return (
            remote(end_out.at[rows, :, packed], even.at[padded, pl.ds(1 + ni * y_lo, ni)], in_send.at[0, block], in_recv.at[0, block], peer_p),
            remote(run_out.at[rows, :, packed], crowd.at[rows, pl.ds(ni * y_lo, ni)], in_send.at[1, block], in_recv.at[1, block], peer_p),
        )

    def start_give(block):
        for copy in give(block):
            copy.start()

    def face_copies(t, block):
        state, par, j = states[t % 2], t % 2, first(block)
        rows, padded = pl.ds(j, ROWS), pl.ds(j + 1, ROWS)
        return (
            remote(state.at[padded, 1], state.at[padded, wide + 1], z_send.at[par, 0, block], z_recv.at[par, 0, block], peer_z),
            remote(state.at[padded, wide], state.at[padded, 0], z_send.at[par, 1, block], z_recv.at[par, 1, block], peer_z),
            remote(edge.at[par, 0, rows], ghost.at[par, 1, rows], k_send.at[par, 0, block], k_recv.at[par, 0, block], peer_k[0]),
            remote(edge.at[par, 1, rows], ghost.at[par, 0, rows], k_send.at[par, 1, block], k_recv.at[par, 1, block], peer_k[1]),
        )

    def row_copy(t, side):
        state, par = states[t % 2], t % 2
        inner = pl.ds(1, wide)
        if side == 0:
            row, ring_row, peer = 1 + (1 - core) * (nj - 1), core * (nj + 1), peer_c
        else:
            row, ring_row, peer = 1 + core * (nj - 1), (1 - core) * (nj + 1), peer_j
        return remote(state.at[row, inner], state.at[ring_row, inner], j_send.at[par, side], j_recv.at[par, side], peer)

    def send_faces(t, block):
        for copy in face_copies(t, block):
            copy.start()

        @pl.when(block == 0)
        def _():
            row_copy(t, 0).start()

        @pl.when(block == blocks - 1)
        def _():
            row_copy(t, 1).start()

    def wait_faces(t, block):
        for copy in face_copies(t, block):
            copy.wait_recv()

        @pl.when(block == 0)
        def _():
            row_copy(t, 0).wait_recv()

        @pl.when(block == blocks - 1)
        def _():
            row_copy(t, 1).wait_recv()

    def sent_faces(t, block):
        for copy in face_copies(t, block):
            copy.wait_send()

        @pl.when(block == 0)
        def _():
            row_copy(t, 0).wait_send()

        @pl.when(block == blocks - 1)
        def _():
            row_copy(t, 1).wait_send()

    def arrive(block):
        for copy in give(block):
            copy.wait_recv()
        for row in range(ROWS):
            j = first(block) + row
            for i in range(wide):
                edge[0, 0, j, i : i + 1, :] = even[j + 1, i + 1, 0:1, :]
                edge[0, 1, j, i : i + 1, :] = even[j + 1, i + 1, half - 1 : half, :]
        send_faces(0, block)

    def step(t, block):
        old, new, par = states[(t - 1) % 2], states[t % 2], (t - 1) % 2
        wait_faces(t - 1, block)
        if t >= 2:
            sent_faces(t - 2, block)
        for row in range(ROWS):
            j = first(block) + row
            r = j + 1
            ends = swing(jnp.where(left, edge[par, 1, j], ghost[par, 0, j]))
            starts = swing(jnp.where(left, ghost[par, 1, j], edge[par, 0, j]))
            lower, middle = old[r, 0], old[r, 1]
            for i in range(wide):
                upper = old[r, i + 2]
                low = jnp.where(place == 0, ends[i : i + 1], pltpu.roll(middle, 1, 0))
                high = jnp.where(place == half - 1, starts[i : i + 1], pltpu.roll(middle, half - 1, 0))
                around = (lower + upper) + (old[r - 1, i + 1] + old[r + 1, i + 1]) + (low + high)
                value = 0.1 * around + middle * (0.6 - 0.2 * (crowd[j, i] * middle))
                new[r, i + 1] = value
                if t < STEPS:
                    edge[t % 2, 0, j, i : i + 1, :] = value[0:1]
                    edge[t % 2, 1, j, i : i + 1, :] = value[half - 1 : half]
                lower, middle = middle, upper
        if t < STEPS:
            send_faces(t, block)

    final = states[STEPS % 2]

    def out_copy(block):
        j = first(block)
        theirs = pl.ds(1 + ni * (1 - y_lo), ni)
        return remote(final.at[pl.ds(j + 1, ROWS), theirs], end_out.at[pl.ds(j, ROWS), :, pl.ds(half, half)], out_send.at[block], out_recv.at[block], peer_p)

    def total_copy(block):
        rows = pl.ds(first(block), ROWS)
        return remote(totals.at[rows], below.at[rows], total_send.at[block], total_recv.at[block], peer_z)

    def base_copy(block):
        rows = pl.ds(first(block), ROWS)
        return remote(bases.at[0, rows], bases.at[1, rows], base_send.at[block], base_recv.at[block], peer_p)

    def finish(block):
        out_copy(block).start()

        @pl.when(z_hi == 0)
        def _():
            for row in range(ROWS):
                j = first(block) + row
                total = final[j + 1, 1]
                for i in range(1, wide):
                    total = total + final[j + 1, i + 1]
                totals[j] = total
                below[j] = jnp.zeros_like(total)
            total_copy(block).start()

    def sums(block):
        @pl.when(z_hi == 1)
        def _():
            total_copy(block).wait_recv()

        sent_faces(STEPS - 1, block)
        for row in range(ROWS):
            j = first(block) + row
            base = below[j]
            lowest = final[j + 1, 1]
            for i in range(1, ni):
                lowest = lowest + final[j + 1, i + 1]
            bases[0, j] = base + jnp.where(y_lo == 0, lowest, 0.0)
            bases[2, j] = base + jnp.where(y_lo == 1, lowest, 0.0)
        base_copy(block).start()

    def returned(block):
        out_copy(block).wait_recv()
        base_copy(block).wait_recv()
        for copy in give(block):
            copy.wait_send()
        scale = 1.0 / (ni * n_lon)
        for row in range(ROWS):
            j = first(block) + row
            run, run_pair = bases[2, j], bases[1, j]
            for q in range(ni):
                value, value_pair = final[j + 1, 1 + ni * y_lo + q], end_out[j, q, half:nk]
                run, run_pair = run + value, run_pair + value_pair
                end_out[j, q, here] = jnp.where(mine, value, swing(value_pair))
                end_out[j, q, away] = jnp.where(mine, swing(value), value_pair)
                scaled, scaled_pair = run * scale, run_pair * scale
                run_out[j, q, here] = jnp.where(mine, scaled, swing(scaled_pair))
                run_out[j, q, away] = jnp.where(mine, swing(scaled), scaled_pair)

    def guarded(stage, block):
        @pl.when((block >= 0) & (block < blocks))
        def _():
            stage(block)

    def close(block):
        out_copy(block).wait_send()
        base_copy(block).wait_send()

        @pl.when(z_hi == 0)
        def _():
            total_copy(block).wait_send()

    def prepare(n, carry):
        guarded(start_give, n)
        guarded(start_load, n + LOADS)
        guarded(pack, n + 1)
        return carry

    lax.fori_loop(0, LOADS, lambda n, carry: (start_load(n), carry)[1], 0)
    pack(0)
    pl.semaphore_wait(barrier, len(peers))
    lax.fori_loop(0, AHEAD, prepare, 0)

    def tick(n, carry):
        prepare(n + AHEAD, 0)
        guarded(returned, n - LAG * STEPS - 2 * LAST)
        guarded(sums, n - LAG * STEPS - LAST)

        def last(block):
            step(STEPS, block)
            finish(block)

        guarded(last, n - LAG * STEPS)
        for t in range(STEPS - 1, 0, -1):
            guarded(lambda block, t=t: step(t, block), n - LAG * t)
        guarded(arrive, n)
        return carry

    lax.fori_loop(0, blocks + LAG * STEPS + 2 * LAST, tick, 0)
    lax.fori_loop(0, blocks, lambda n, _: (close(n), 0)[1], 0)


def flush_kernel(run_in, end_in, run_out, end_out, sems):
    copies = []
    for k in range(PIECES):
        size = run_in.shape[0] // PIECES
        rows = pl.ds(k * size, size)
        copies.append(pltpu.make_async_copy(run_in.at[rows], run_out.at[rows], sems.at[0, k]))
        copies.append(pltpu.make_async_copy(end_in.at[rows], end_out.at[rows], sems.at[1, k]))
    for copy in copies:
        copy.start()
    for copy in copies:
        copy.wait()


def solution(mesh):
    n_lat, n_lon, n_lev = (mesh.shape[axis] for axis in ("lat", "lon", "lev"))

    def body(density, crowding):
        nj, ni, nk, cells = density.shape
        half, blocks, wide = nk // 2, nj // ROWS, 2 * ni
        f32, dma = jnp.float32, pltpu.SemaphoreType.DMA
        out = pltpu.VMEM(density.shape, f32)
        vmem = [
            (nj + 2, wide + 2, half, cells),
            (nj + 2, wide + 2, half, cells),
            (nj, wide, half, cells),
            (2, 2, nj, wide, cells),
            (2, 2, nj, wide, cells),
            (nj, half, cells),
            (nj, half, cells),
            (3, nj, half, cells),
        ]
        sems = [
            (2, 2, blocks), (2, 2, blocks), (2, 2, blocks), (2, 2, blocks), (2, 2), (2, 2),
            (2, blocks), (2, blocks), (2, blocks), (blocks,), (blocks,), (blocks,), (blocks,),
            (blocks,), (blocks,),
        ]
        sizes = (n_lat, n_lon, n_lev, nj, ni, nk, cells)
        anywhere = pl.BlockSpec(memory_space=pl.ANY)
        inside = pl.BlockSpec(memory_space=pltpu.VMEM)

        def kernel(*refs):
            swap_kernel(sizes, *refs)

        results = pl.pallas_call(
            kernel,
            out_shape=(out, out),
            in_specs=[anywhere, anywhere],
            out_specs=(inside, inside),
            scratch_shapes=[pltpu.VMEM(shape, f32) for shape in vmem] + [dma(shape) for shape in sems],
            compiler_params=pltpu.CompilerParams(
                collective_id=0, has_side_effects=True, vmem_limit_bytes=47 * 1024 * 1024
            ),
            cost_estimate=pl.CostEstimate(flops=14 * STEPS * density.size, bytes_accessed=16 * density.size, transcendentals=0),
            name="swap_sweep",
        )(density, crowding)
        whole = jax.ShapeDtypeStruct(density.shape, f32)
        return pl.pallas_call(
            flush_kernel,
            out_shape=(whole, whole),
            in_specs=[inside, inside],
            out_specs=(anywhere, anywhere),
            scratch_shapes=[dma((2, PIECES))],
            compiler_params=pltpu.CompilerParams(vmem_limit_bytes=1024 * 1024),
            cost_estimate=pl.CostEstimate(flops=density.size, bytes_accessed=16 * density.size, transcendentals=0),
            name="flush",
        )(*results)

    spec = P("lat", "lon", "lev", None)
    return jax.shard_map(body, mesh=mesh, in_specs=(spec, spec), out_specs=(spec, spec), check_vma=False)
```

```python
import jax
import jax.numpy as jnp
from jax import lax
from jax.experimental import pallas as pl
from jax.experimental.pallas import tpu as pltpu
from jax.sharding import PartitionSpec as P

STEPS = 4
ROWS = 2
LAG = 2
LAST = 1
HOP = 2
PLAIN = 6
AHEAD = 1
PIECES = 4
LOADS = 4
MESH = pl.DeviceIdType.MESH


def swap_kernel(
    sizes,
    d_hbm, c_hbm, run_out, end_out,
    even, odd, crowd, ghost, edge, below, totals, bases, relay,
    z_send, z_recv, k_send, k_recv, j_send, j_recv,
    in_send, in_recv, in_own, out_send, out_recv, base_send, base_recv,
    relay_send, relay_recv, total_send, total_recv,
):
    n_lat, n_lon, n_lev, nj, ni, nk, cells = sizes
    half, blocks = nk // 2, nj // ROWS
    wide = 2 * ni
    a, b, m = lax.axis_index("lat"), lax.axis_index("lon"), lax.axis_index("lev")
    core, y_hi = lax.rem(a, 2), a // 2
    y_lo, z_hi = lax.rem(b, 2), b // 2
    h = lax.rem(y_lo + y_hi, 2)
    pair = b + 1 - 2 * y_lo
    peer_p = (a, pair, m)
    peer_z = (a, lax.rem(b + 2, n_lon), m)
    peer_k = ((a, b, lax.rem(m + n_lev - 1, n_lev)), (a, b, lax.rem(m + 1, n_lev)))
    peer_c = (a + 1 - 2 * core, b, m)
    peer_j = (lax.rem(a + n_lat - 1 + 2 * core, n_lat), pair, m)
    states = (even, odd)

    barrier = pltpu.get_barrier_semaphore()
    peers = (peer_p, peer_z, *peer_k, peer_c, peer_j)
    for peer in peers:
        pl.semaphore_signal(barrier, inc=1, device_id=peer, device_id_type=MESH)

    def first(block):
        return block * ROWS + (1 - core) * (nj - (2 * block + 1) * ROWS)

    def remote(src, dst, send, recv, peer):
        return pltpu.make_async_remote_copy(
            src_ref=src, dst_ref=dst, send_sem=send, recv_sem=recv,
            device_id=peer, device_id_type=MESH,
        )

    here = pl.ds(pl.multiple_of(half * h, 8), half)
    away = pl.ds(pl.multiple_of(half * (1 - h), 8), half)
    lane = lax.broadcasted_iota(jnp.int32, (half, cells), 1)
    mine = jnp.where(lane >= cells // 2, 1, 0) == h
    place = lax.broadcasted_iota(jnp.int32, (half, cells), 0)
    left = lax.broadcasted_iota(jnp.int32, (wide, cells), 1) < cells // 2

    def swing(value):
        return pltpu.roll(value, cells // 2, 1)

    def load(block):
        rows = pl.ds(first(block), ROWS)
        return (
            pltpu.make_async_copy(d_hbm.at[rows], end_out.at[rows], in_own.at[0, block]),
            pltpu.make_async_copy(c_hbm.at[rows], run_out.at[rows], in_own.at[1, block]),
        )

    def start_load(block):
        for copy in load(block):
            copy.start()

    def pack(block):
        for copy in load(block):
            copy.wait()
        for row in range(ROWS):
            j = first(block) + row
            for q in range(ni):
                for source, kept in (
                    (end_out, even.at[j + 1, 1 + ni * y_lo + q]),
                    (run_out, crowd.at[j, ni * y_lo + q]),
                ):
                    near, far = source[j, q, here], source[j, q, away]
                    kept[...] = jnp.where(mine, near, swing(far))
                    source[j, q, 0:half] = jnp.where(mine, swing(near), far)

    def give(block):
        j = first(block)
        rows, padded = pl.ds(j, ROWS), pl.ds(j + 1, ROWS)
        packed = pl.ds(0, half)
        return (
            remote(end_out.at[rows, :, packed], even.at[padded, pl.ds(1 + ni * y_lo, ni)], in_send.at[0, block], in_recv.at[0, block], peer_p),
            remote(run_out.at[rows, :, packed], crowd.at[rows, pl.ds(ni * y_lo, ni)], in_send.at[1, block], in_recv.at[1, block], peer_p),
        )

    def start_give(block):
        for copy in give(block):
            copy.start()

    def face_copies(t, block):
        state, par, j = states[t % 2], t % 2, first(block)
        rows, padded = pl.ds(j, ROWS), pl.ds(j + 1, ROWS)
        return (
            remote(state.at[padded, 1], state.at[padded, wide + 1], z_send.at[par, 0, block], z_recv.at[par, 0, block], peer_z),
            remote(state.at[padded, wide], state.at[padded, 0], z_send.at[par, 1, block], z_recv.at[par, 1, block], peer_z),
            remote(edge.at[par, 0, rows], ghost.at[par, 1, rows], k_send.at[par, 0, block], k_recv.at[par, 0, block], peer_k[0]),
            remote(edge.at[par, 1, rows], ghost.at[par, 0, rows], k_send.at[par, 1, block], k_recv.at[par, 1, block], peer_k[1]),
        )

    def row_copy(t, side):
        state, par = states[t % 2], t % 2
        inner = pl.ds(1, wide)
        if side == 0:
            row, ring_row, peer = 1 + (1 - core) * (nj - 1), core * (nj + 1), peer_c
        else:
            row, ring_row, peer = 1 + core * (nj - 1), (1 - core) * (nj + 1), peer_j
        return remote(state.at[row, inner], state.at[ring_row, inner], j_send.at[par, side], j_recv.at[par, side], peer)

    def send_faces(t, block):
        for copy in face_copies(t, block):
            copy.start()

        @pl.when(block == 0)
        def _():
            row_copy(t, 0).start()

        @pl.when(block == blocks - 1)
        def _():
            row_copy(t, 1).start()

    def wait_faces(t, block):
        for copy in face_copies(t, block):
            copy.wait_recv()

        @pl.when(block == 0)
        def _():
            row_copy(t, 0).wait_recv()

        @pl.when(block == blocks - 1)
        def _():
            row_copy(t, 1).wait_recv()

    def sent_faces(t, block):
        for copy in face_copies(t, block):
            copy.wait_send()

        @pl.when(block == 0)
        def _():
            row_copy(t, 0).wait_send()

        @pl.when(block == blocks - 1)
        def _():
            row_copy(t, 1).wait_send()

    def arrive(block):
        for copy in give(block):
            copy.wait_recv()
        for row in range(ROWS):
            j = first(block) + row
            for i in range(wide):
                edge[0, 0, j, i : i + 1, :] = even[j + 1, i + 1, 0:1, :]
                edge[0, 1, j, i : i + 1, :] = even[j + 1, i + 1, half - 1 : half, :]
        send_faces(0, block)

    def step(t, block):
        old, new, par = states[(t - 1) % 2], states[t % 2], (t - 1) % 2
        wait_faces(t - 1, block)
        if t >= 2:
            sent_faces(t - 2, block)
        for row in range(ROWS):
            j = first(block) + row
            r = j + 1
            ends = swing(jnp.where(left, edge[par, 1, j], ghost[par, 0, j]))
            starts = swing(jnp.where(left, ghost[par, 1, j], edge[par, 0, j]))
            lower, middle = old[r, 0], old[r, 1]
            for i in range(wide):
                upper = old[r, i + 2]
                low = jnp.where(place == 0, ends[i : i + 1], pltpu.roll(middle, 1, 0))
                high = jnp.where(place == half - 1, starts[i : i + 1], pltpu.roll(middle, half - 1, 0))
                around = (lower + upper) + (old[r - 1, i + 1] + old[r + 1, i + 1]) + (low + high)
                value = 0.1 * around + middle * (0.6 - 0.2 * (crowd[j, i] * middle))
                new[r, i + 1] = value
                if t < STEPS:
                    edge[t % 2, 0, j, i : i + 1, :] = value[0:1]
                    edge[t % 2, 1, j, i : i + 1, :] = value[half - 1 : half]
                lower, middle = middle, upper
        if t < STEPS:
            send_faces(t, block)

    final = states[STEPS % 2]

    def out_copy(block):
        j = first(block)
        theirs = pl.ds(1 + ni * (1 - y_lo), ni)
        return remote(final.at[pl.ds(j + 1, ROWS), theirs], end_out.at[pl.ds(j, ROWS), :, pl.ds(half, half)], out_send.at[block], out_recv.at[block], peer_p)

    def slot(block):
        return pl.ds(block * ROWS, ROWS)

    def total_copy(block):
        rows = slot(block)
        return remote(totals.at[rows], below.at[rows], total_send.at[block], total_recv.at[block], peer_z)

    far, not_far = pl.ds(0, half // 4), pl.ds(half // 4, half - half // 4)
    aside, not_aside = pl.ds(0, half // 2), pl.ds(half // 2, half - half // 2)
    up, down = y_lo == 0, y_lo == 1
    base_from, base_to = bases.at[0], bases.at[1]

    def base_copy(block, part, source, target, which, arrival, peer):
        rows = slot(block)
        return remote(source.at[rows, part], target.at[rows, part], base_send.at[which, block], arrival, peer)

    def relay_copy(block, part, target, which, arrival, peer):
        rows = slot(block)
        return remote(relay.at[which, rows, part], target.at[rows, part], relay_send.at[which, block], arrival, peer)

    def give_base_split(block):
        @pl.when(up)
        def _():
            base_copy(block, far, base_from, relay.at[0], 1, relay_recv.at[0, block], peer_j).start()
            base_copy(block, not_far, base_from, base_to, 0, base_recv.at[0, block], peer_p).start()

        @pl.when(down & (z_hi == 1))
        def _():
            base_copy(block, not_aside, base_from, base_to, 0, base_recv.at[0, block], peer_p).start()

        @pl.when(down & (z_hi == 0))
        def _():
            base_copy(block, aside, totals, relay.at[1], 1, relay_recv.at[1, block], peer_p).start()

    def relay_first(block):
        @pl.when(down)
        def _():
            copy = relay_copy(block, far, relay.at[0], 0, relay_recv.at[0, block], peer_p)
            copy.wait_recv()
            copy.start()

        @pl.when(up & (z_hi == 0))
        def _():
            relay_copy(block, aside, relay.at[1], 1, relay_recv.at[1, block], peer_p).wait_recv()
            relay_copy(block, aside, base_to, 1, base_recv.at[1, block], peer_z).start()

    def relay_second(block):
        @pl.when(up)
        def _():
            relay_copy(block, far, relay.at[0], 0, relay_recv.at[0, block], peer_p).wait_recv()
            relay_copy(block, far, base_to, 0, base_recv.at[1, block], peer_j).start()

    def wait_base_split(block):
        @pl.when(down)
        def _():
            base_copy(block, not_far, base_from, base_to, 0, base_recv.at[0, block], peer_p).wait_recv()
            base_copy(block, far, base_from, base_to, 0, base_recv.at[1, block], peer_p).wait_recv()

        @pl.when(up & (z_hi == 1))
        def _():
            base_copy(block, not_aside, base_from, base_to, 0, base_recv.at[0, block], peer_p).wait_recv()
            base_copy(block, aside, base_from, base_to, 0, base_recv.at[1, block], peer_p).wait_recv()

    def sent_base_split(block):
        relay_copy(block, far, relay.at[0], 0, relay_recv.at[0, block], peer_p).wait_send()

        @pl.when(up)
        def _():
            base_copy(block, not_far, base_from, base_to, 0, base_recv.at[0, block], peer_p).wait_send()
            base_copy(block, far, base_from, base_to, 1, base_recv.at[0, block], peer_p).wait_send()

        @pl.when(up & (z_hi == 0))
        def _():
            relay_copy(block, aside, relay.at[1], 1, relay_recv.at[1, block], peer_p).wait_send()

        @pl.when(down & (z_hi == 1))
        def _():
            base_copy(block, not_aside, base_from, base_to, 0, base_recv.at[0, block], peer_p).wait_send()

        @pl.when(down & (z_hi == 0))
        def _():
            base_copy(block, aside, base_from, base_to, 1, base_recv.at[0, block], peer_p).wait_send()

    every = pl.ds(0, half)

    def give_base_plain(block):
        @pl.when(up | (z_hi == 1))
        def _():
            base_copy(block, every, base_from, base_to, 0, base_recv.at[0, block], peer_p).start()

    def wait_base_plain(block):
        @pl.when(down | (z_hi == 1))
        def _():
            base_copy(block, every, base_from, base_to, 0, base_recv.at[0, block], peer_p).wait_recv()

    def sent_base_plain(block):
        @pl.when(up | (z_hi == 1))
        def _():
            base_copy(block, every, base_from, base_to, 0, base_recv.at[0, block], peer_p).wait_send()

    def either(split, plain, block):
        @pl.when(block < blocks - PLAIN)
        def _():
            split(block)

        @pl.when(block >= blocks - PLAIN)
        def _():
            plain(block)

    def give_base(block):
        either(give_base_split, give_base_plain, block)

    def wait_base(block):
        either(wait_base_split, wait_base_plain, block)

    def sent_base(block):
        either(sent_base_split, sent_base_plain, block)

    def finish(block):
        out_copy(block).start()

        @pl.when(z_hi == 0)
        def _():
            for row in range(ROWS):
                j = first(block) + row
                total = final[j + 1, 1]
                for i in range(1, wide):
                    total = total + final[j + 1, i + 1]
                totals[block * ROWS + row] = total
                below[block * ROWS + row] = jnp.zeros_like(total)
            total_copy(block).start()

        @pl.when(up & (z_hi == 0))
        def _():
            bases[1, slot(block)] = jnp.zeros((ROWS, half, cells), jnp.float32)

    def sums(block):
        @pl.when(z_hi == 1)
        def _():
            total_copy(block).wait_recv()

        sent_faces(STEPS - 1, block)
        for row in range(ROWS):
            j = first(block) + row
            base = below[block * ROWS + row]
            lowest = final[j + 1, 1]
            for i in range(1, ni):
                lowest = lowest + final[j + 1, i + 1]
            bases[0, block * ROWS + row] = base + jnp.where(y_lo == 0, lowest, 0.0)
            bases[2, block * ROWS + row] = base + jnp.where(y_lo == 1, lowest, 0.0)
        give_base(block)

    def returned(block):
        out_copy(block).wait_recv()
        wait_base(block)
        for copy in give(block):
            copy.wait_send()
        scale = 1.0 / (ni * n_lon)
        for row in range(ROWS):
            j = first(block) + row
            run, run_pair = bases[2, block * ROWS + row], bases[1, block * ROWS + row]
            for q in range(ni):
                value, value_pair = final[j + 1, 1 + ni * y_lo + q], end_out[j, q, half:nk]
                run, run_pair = run + value, run_pair + value_pair
                end_out[j, q, here] = jnp.where(mine, value, swing(value_pair))
                end_out[j, q, away] = jnp.where(mine, swing(value), value_pair)
                scaled, scaled_pair = run * scale, run_pair * scale
                run_out[j, q, here] = jnp.where(mine, scaled, swing(scaled_pair))
                run_out[j, q, away] = jnp.where(mine, swing(scaled), scaled_pair)

    def guarded(stage, block, start=0, stop=blocks):
        @pl.when((block >= start) & (block < stop))
        def _():
            stage(block)

    def close(block):
        out_copy(block).wait_send()
        sent_base(block)

        @pl.when(z_hi == 0)
        def _():
            total_copy(block).wait_send()

    def prepare(n, carry):
        guarded(start_give, n)
        guarded(start_load, n + LOADS)
        guarded(pack, n + 1)
        return carry

    lax.fori_loop(0, LOADS, lambda n, carry: (start_load(n), carry)[1], 0)
    pack(0)
    pl.semaphore_wait(barrier, len(peers))
    lax.fori_loop(0, AHEAD, prepare, 0)

    def tick(n, carry):
        prepare(n + AHEAD, 0)
        done = n - LAG * STEPS - LAST
        split = blocks - PLAIN
        guarded(relay_second, done - 2 * HOP, stop=split)
        guarded(relay_first, done - HOP, stop=split)
        guarded(returned, done - 3 * HOP, stop=split)
        guarded(returned, done - LAST, start=split)
        guarded(sums, n - LAG * STEPS - LAST)

        def last(block):
            step(STEPS, block)
            finish(block)

        guarded(last, n - LAG * STEPS)
        for t in range(STEPS - 1, 0, -1):
            guarded(lambda block, t=t: step(t, block), n - LAG * t)
        guarded(arrive, n)
        return carry

    lax.fori_loop(0, blocks + LAG * STEPS + LAST + max(LAST, 3 * HOP - PLAIN), tick, 0)
    lax.fori_loop(0, blocks, lambda n, _: (close(n), 0)[1], 0)


def flush_kernel(run_in, end_in, run_out, end_out, sems):
    copies = []
    for k in range(PIECES):
        size = run_in.shape[0] // PIECES
        rows = pl.ds(k * size, size)
        copies.append(pltpu.make_async_copy(run_in.at[rows], run_out.at[rows], sems.at[0, k]))
        copies.append(pltpu.make_async_copy(end_in.at[rows], end_out.at[rows], sems.at[1, k]))
    for copy in copies:
        copy.start()
    for copy in copies:
        copy.wait()


def solution(mesh):
    n_lat, n_lon, n_lev = (mesh.shape[axis] for axis in ("lat", "lon", "lev"))

    def body(density, crowding):
        nj, ni, nk, cells = density.shape
        half, blocks, wide = nk // 2, nj // ROWS, 2 * ni
        f32, dma = jnp.float32, pltpu.SemaphoreType.DMA
        out = pltpu.VMEM(density.shape, f32)
        vmem = [
            (nj + 2, wide + 2, half, cells),
            (nj + 2, wide + 2, half, cells),
            (nj, wide, half, cells),
            (2, 2, nj, wide, cells),
            (2, 2, nj, wide, cells),
            (nj, half, cells),
            (nj, half, cells),
            (3, nj, half, cells),
            (2, nj, half, cells),
        ]
        sems = [
            (2, 2, blocks), (2, 2, blocks), (2, 2, blocks), (2, 2, blocks), (2, 2), (2, 2),
            (2, blocks), (2, blocks), (2, blocks), (blocks,), (blocks,), (2, blocks), (2, blocks),
            (2, blocks), (2, blocks), (blocks,), (blocks,),
        ]
        sizes = (n_lat, n_lon, n_lev, nj, ni, nk, cells)
        anywhere = pl.BlockSpec(memory_space=pl.ANY)
        inside = pl.BlockSpec(memory_space=pltpu.VMEM)

        def kernel(*refs):
            swap_kernel(sizes, *refs)

        results = pl.pallas_call(
            kernel,
            out_shape=(out, out),
            in_specs=[anywhere, anywhere],
            out_specs=(inside, inside),
            scratch_shapes=[pltpu.VMEM(shape, f32) for shape in vmem] + [dma(shape) for shape in sems],
            compiler_params=pltpu.CompilerParams(
                collective_id=0, has_side_effects=True, vmem_limit_bytes=47 * 1024 * 1024
            ),
            cost_estimate=pl.CostEstimate(flops=14 * STEPS * density.size, bytes_accessed=16 * density.size, transcendentals=0),
            name="swap_sweep",
        )(density, crowding)
        whole = jax.ShapeDtypeStruct(density.shape, f32)
        return pl.pallas_call(
            flush_kernel,
            out_shape=(whole, whole),
            in_specs=[inside, inside],
            out_specs=(anywhere, anywhere),
            scratch_shapes=[dma((2, PIECES))],
            compiler_params=pltpu.CompilerParams(vmem_limit_bytes=1024 * 1024),
            cost_estimate=pl.CostEstimate(flops=density.size, bytes_accessed=16 * density.size, transcendentals=0),
            name="flush",
        )(*results)

    spec = P("lat", "lon", "lev", None)
    return jax.shard_map(body, mesh=mesh, in_specs=(spec, spec), out_specs=(spec, spec), check_vma=False)
```
